32 devices in a mesh: dp: 8 (over z, y), tensor: 4 (over x, core).
Axes of the slice: x: 2, y: 2, z: 4, core: 2. Of those that a mesh axis runs over, the one named last changes fastest.
Arguments:
- tokens: bfloat16 [16384, 768], P(('dp', 'tensor')), may hold values from -6 to 6
- seq_lengths: int32 [16], P('dp'), may hold values from 100 to 1024, as said below
- cotangent: bfloat16 [16384, 768], P(('dp', 'tensor')), may hold values from -6 to 6
- ln1_gain: bfloat16 [768], replicated, may hold values from 0.5 to 1.5
- ln1_shift: bfloat16 [768], replicated, may hold values from -2 to 2
- w_qkv: bfloat16 [768, 3, 768], P(None, None, 'tensor'), may hold values from -0.21875 to 0.21875
- b_qkv: bfloat16 [3, 768], P(None, 'tensor'), may hold values from -2 to 2
- w_out: bfloat16 [768, 768], P('tensor'), may hold values from -1.25 to 1.25
- b_out: bfloat16 [768], replicated, may hold values from -2 to 2
- ln2_gain: bfloat16 [768], replicated, may hold values from 0.5 to 1.5
- ln2_shift: bfloat16 [768], replicated, may hold values from -2 to 2
- w_up: bfloat16 [768, 3072], P(None, 'tensor'), may hold values from -0.21875 to 0.21875
- b_up: bfloat16 [3072], P('tensor'), may hold values from -2 to 2
- w_down: bfloat16 [3072, 768], P('tensor'), may hold values from -0.109375 to 0.109375
- b_down: bfloat16 [768], replicated, may hold values from -2 to 2
Outputs:
- output: bfloat16 [16384, 768], P(('dp', 'tensor'))
- grad_tokens: bfloat16 [16384, 768], P(('dp', 'tensor'))
- grad_ln1_gain: float32 [768], replicated
- grad_ln1_shift: float32 [768], replicated
- grad_w_qkv: float32 [768, 3, 768], P(None, None, 'tensor')
- grad_b_qkv: float32 [3, 768], P(None, 'tensor')
- grad_w_out: float32 [768, 768], P('tensor')
- grad_b_out: float32 [768], replicated
- grad_ln2_gain: float32 [768], replicated
- grad_ln2_shift: float32 [768], replicated
- grad_w_up: float32 [768, 3072], P(None, 'tensor')
- grad_b_up: float32 [3072], P('tensor')
- grad_w_down: float32 [3072, 768], P('tensor')
- grad_b_down: float32 [768], replicated
The draws below stay inside these ranges and needn't reach their ends.
Inputs may be any that keep to these rules, and one draw needn't show every extreme that they name: `seq_lengths`: number of codons of each sequence; one sequence has exactly 1024 and one exactly 100; short sequences are more common than long ones.
All inputs are finite; a program needn't handle non-finite values.
Results may differ from the reference program's by a relative error of at most 0.013.
Values may be sent and summed in bfloat16 or wider, within the bound.
A program may use at most 128 MiB of HBM per device.

```python
import math
import jax
import jax.numpy as jnp
from jax import lax

D = 768
HEADS = 12
HEAD_DIM = 64
FF = 3072
SEQ = 1024
MIN_LEN = 100
SEQ_DEV = 2
SEQS = 16
TOKENS = 16384


def draw_seq_lengths(key, part):
    first_key, second_key = jax.random.split(key)
    first_draw = jax.random.randint(first_key, (SEQS,), MIN_LEN, SEQ + 1)
    second_draw = jax.random.randint(second_key, (SEQS,), MIN_LEN, SEQ + 1)
    lengths_out = jnp.minimum(first_draw, second_draw)
    lengths_out = lengths_out.at[0].set(SEQ).at[1].set(MIN_LEN)
    return lengths_out.astype(jnp.int32)


def level_of(stream_key, extent, pieces, low, largest):
    loudness, own = 1.0, jax.random.fold_in(stream_key, 6)
    for dim, shards_of in pieces:
        draws = jnp.exp(jax.random.uniform(jax.random.fold_in(own, dim), (shards_of,), jnp.float32, low / len(pieces), largest / len(pieces)))
        loudness = loudness * jnp.repeat(draws, extent[dim] // shards_of).reshape([-1 if axis == dim else 1 for axis in range(len(extent))])
    return loudness


def normal_values(rng, extent, width, most, cuts=(), held_as=jnp.bfloat16):
    level = level_of(rng, extent, cuts, -0.22, 0.18) if cuts else 1.0
    array = jax.random.normal(rng, extent, jnp.float32) * width * level
    return jnp.minimum(jnp.maximum(array, -most), most).astype(held_as)


def setup_inputs(seed: int = 0) -> dict:
    arg_keys = jax.random.split(jax.random.key(seed), 16)
    return {
        "tokens": normal_values(arg_keys[0], (TOKENS, D), 1.0, 6.0, ((0, 32),)),
        "seq_lengths": draw_seq_lengths(jax.random.fold_in(arg_keys[15], 71), 0),
        "cotangent": normal_values(arg_keys[2], (TOKENS, D), 1.0, 6.0, ((0, 32),)),
        "ln1_gain": jnp.clip(1.0 + 0.1 * jax.random.normal(arg_keys[3], (D,), jnp.float32), 0.5, 1.5).astype(jnp.bfloat16),
        "ln1_shift": normal_values(arg_keys[4], (D,), 0.3, 2.0),
        "w_qkv": normal_values(arg_keys[5], (D, 3, D), D ** -0.5, 0.21875, ((2, 4),)),
        "b_qkv": normal_values(arg_keys[6], (3, D), 0.3, 2.0, ((1, 4),)),
        "w_out": normal_values(arg_keys[7], (D, D), (D // 32) ** -0.5, 1.25, ((0, 4),)),
        "b_out": normal_values(arg_keys[8], (D,), 0.3, 2.0),
        "ln2_gain": jnp.clip(1.0 + 0.1 * jax.random.normal(arg_keys[9], (D,), jnp.float32), 0.5, 1.5).astype(jnp.bfloat16),
        "ln2_shift": normal_values(arg_keys[10], (D,), 0.3, 2.0),
        "w_up": normal_values(arg_keys[11], (D, FF), D ** -0.5, 0.21875, ((1, 4),)),
        "b_up": normal_values(arg_keys[12], (FF,), 0.3, 2.0, ((0, 4),)),
        "w_down": normal_values(arg_keys[13], (FF, D), FF ** -0.5, 0.109375, ((0, 4),)),
        "b_down": normal_values(arg_keys[14], (D,), 0.3, 2.0),
    }


@jax.custom_vjp
def low(v):
    return lax.optimization_barrier(v.astype(jnp.bfloat16)).astype(jnp.float32)

@jax.custom_vjp
def low_back(v):
    return v

def low_keep(v):
    return (low(v), None)

def low_pass(kept, grad):
    return (grad,)

def back_keep(v):
    return (v, None)

def back_low(kept, grad):
    return (low(grad),)
low.defvjp(low_keep, low_pass)
low_back.defvjp(back_keep, back_low)
norm_eps = 1e-05
mask_fill = -1e+30
highest = lax.Precision.HIGHEST

def layer_norm(values, ln_gain, ln_shift):
    row_mean = lax.optimization_barrier(jnp.mean(values, axis=-1, keepdims=True))
    centred = values - row_mean
    row_var = lax.optimization_barrier(jnp.mean(centred * centred, axis=-1, keepdims=True))
    return centred * lax.rsqrt(row_var + norm_eps) * ln_gain + ln_shift

def rotary_tables():
    half_dim = HEAD_DIM // 2
    inverse_freq = jnp.exp(jnp.arange(half_dim, dtype=jnp.float32) * (-2.0 * math.log(10000.0) / HEAD_DIM))
    angles = jnp.arange(SEQ, dtype=jnp.float32)[:, None] * inverse_freq[None, :]
    return (jnp.cos(angles), jnp.sin(angles))

def rotate(head_vals, cosine, sine_table):
    half_dim = head_vals.shape[-1] // 2
    lower_half = head_vals[..., :half_dim]
    upper_half = head_vals[..., half_dim:]
    cos_part = cosine[:, None, :]
    sin_part = sine_table[:, None, :]
    return jnp.concatenate([lower_half * cos_part - upper_half * sin_part, upper_half * cos_part + lower_half * sin_part], axis=-1)

def attend_block(query_blk, key_seq, value_seq, key_valid):
    scores = low_back(jnp.einsum('qhe,khe->hqk', query_blk, key_seq, precision=highest) * HEAD_DIM ** (-0.5))
    scores = jnp.where(key_valid[None, None, :], scores, mask_fill)
    weights = low(jax.nn.softmax(scores, axis=-1))
    return jnp.einsum('hqk,khe->qhe', weights, value_seq, precision=highest)

def attend_seq(inputs):
    query_seq, key_seq, value_seq, seq_len = inputs
    key_valid = jnp.arange(SEQ) < seq_len
    block_rows = min(512, SEQ)
    out_parts = []
    for offset in range(0, SEQ, block_rows):
        out_parts.append(jax.checkpoint(attend_block)(query_seq[offset:offset + block_rows], key_seq, value_seq, key_valid))
    return jnp.concatenate(out_parts, axis=0)

def forward(params_in, values_in, lengths_in):
    gain_one, shift_one, wqkv_in, bqkv_in, wout_in, bout_in, gain_two, shift_two, wup_in, bup_in, wdown_in, bdown_in = params_in
    cosine, sine_table = rotary_tables()
    normed_one = low(layer_norm(values_in, gain_one, shift_one))
    qkv_all = low_back(jnp.einsum('td,dcf->tcf', normed_one, wqkv_in, precision=highest) + bqkv_in)
    query_raw = qkv_all[:, 0].reshape(-1, SEQ, HEADS, HEAD_DIM)
    key_raw = qkv_all[:, 1].reshape(-1, SEQ, HEADS, HEAD_DIM)
    query_low = low(rotate(query_raw, cosine, sine_table))
    key_low = low(rotate(key_raw, cosine, sine_table))
    value_low = low(qkv_all[:, 2].reshape(-1, SEQ, HEADS, HEAD_DIM))
    attended = lax.map(attend_seq, (query_low, key_low, value_low, lengths_in))
    attn_vals = low(low_back(attended.reshape(-1, D)))
    mixed = values_in + low_back(jnp.dot(attn_vals, wout_in, precision=highest)) + bout_in
    normed_two = low(layer_norm(mixed, gain_two, shift_two))
    pre_act = low_back(jnp.dot(normed_two, wup_in, precision=highest) + bup_in)
    act_low = low(jax.nn.gelu(pre_act))
    return mixed + jnp.dot(act_low, wdown_in, precision=highest) + bdown_in

def reference(tokens, seq_lengths, cotangent, ln1_gain, ln1_shift, w_qkv, b_qkv, w_out, b_out, ln2_gain, ln2_shift, w_up, b_up, w_down, b_down):
    params_all = tuple((item.astype(jnp.float32) for item in (ln1_gain, ln1_shift, w_qkv, b_qkv, w_out, b_out, ln2_gain, ln2_shift, w_up, b_up, w_down, b_down)))
    group_count = seq_lengths.shape[0] // SEQ_DEV
    token_groups = tokens.astype(jnp.float32).reshape(group_count, SEQ_DEV * SEQ, D)
    cot_groups = cotangent.astype(jnp.float32).reshape(group_count, SEQ_DEV * SEQ, D)
    length_groups = seq_lengths.reshape(group_count, SEQ_DEV)

    def one_group(totals, item_in):
        group_tokens, group_cot, group_lengths = item_in

        def apply_layer(params_in, values_in):
            return forward(params_in, values_in, group_lengths)
        out_vals, pull_back = jax.vjp(apply_layer, params_all, group_tokens)
        grad_params, grad_values = pull_back(group_cot)
        totals = jax.tree.map(lambda left_val, right_val: left_val + right_val, totals, grad_params)
        return (totals, (out_vals.astype(jnp.bfloat16), grad_values.astype(jnp.bfloat16)))
    zero_grads = jax.tree.map(jnp.zeros_like, params_all)
    grad_sums, (out_groups, grad_groups) = lax.scan(one_group, zero_grads, (token_groups, cot_groups, length_groups))
    output = out_groups.reshape(-1, D)
    grad_tokens = grad_groups.reshape(-1, D)
    return (output, grad_tokens, grad_sums[0], grad_sums[1], grad_sums[2], grad_sums[3], grad_sums[4], grad_sums[5], grad_sums[6], grad_sums[7], grad_sums[8], grad_sums[9], grad_sums[10], grad_sums[11])
```

```python
import functools
import math

import jax
import jax.numpy as jnp
from jax import lax
from jax.experimental import pallas as pl
from jax.experimental.pallas import tpu as pltpu
from jax.sharding import PartitionSpec as P

HEAD_DIM = 64
SEQ = 1024
PAIR = 2 * HEAD_DIM
TILE = 256

norm_eps = 1e-05
mask_fill = -1e30
f32 = jnp.float32
bf16 = jnp.bfloat16


def dot(left, right, left_dim, right_dim):
    return lax.dot_general(
        left, right, (((left_dim,), (right_dim,)), ((), ())), preferred_element_type=f32
    )


def norm_stats(values):
    mean = jnp.mean(values, axis=-1, keepdims=True)
    centred = values - mean
    var = jnp.mean(centred * centred, axis=-1, keepdims=True)
    scale = lax.rsqrt(var + norm_eps)
    return centred * scale, scale


def norm_back(grad, gain, xhat, scale):
    e = grad * gain
    return scale * (
        e
        - jnp.mean(e, axis=-1, keepdims=True)
        - xhat * jnp.mean(e * xhat, axis=-1, keepdims=True)
    )


def swap(array, axis, bit):
    count = lax.axis_size(axis)
    return lax.ppermute(array, axis, [(i, i ^ bit) for i in range(count)])


def bits_of(axis):
    count = lax.axis_size(axis)
    return [1 << i for i in range(count.bit_length() - 1)]


def half_rows(array, which):
    half = array.shape[0] // 2
    return lax.dynamic_slice_in_dim(array, which * half, half, axis=0)


class Sum:
    def __init__(self, array, order):
        self.array = array
        self.todo = [(bit, True) for bit in order] + [(bit, False) for bit in reversed(order)]
        self.flight = None

    def start(self):
        bit, fold = self.todo.pop(0)
        mine = (lax.axis_index("dp") // bit) % 2
        send = half_rows(self.array, 1 - mine) if fold else self.array
        self.flight = (bit, fold, mine, swap(send, "dp", bit))
        return send

    def finish(self):
        bit, fold, mine, got = self.flight
        self.flight = None
        if fold:
            kept = half_rows(self.array, mine)
            self.array = (kept.astype(f32) + got.astype(f32)).astype(bf16)
        else:
            low = jnp.where(mine == 0, self.array, got)
            high = jnp.where(mine == 0, got, self.array)
            self.array = jnp.concatenate([low, high], axis=0)


def advance(sums, *tied):
    sent = []
    for item in sums:
        if item.flight is not None:
            item.finish()
        if item.todo:
            sent.append(item.start())
    held = lax.optimization_barrier((tuple(tied), tuple(sent)))[0]
    return held if len(held) > 1 else held[0]


def key_bias(info_ref, rows):
    length, parity = info_ref[0], info_ref[1]
    pos = lax.broadcasted_iota(jnp.int32, (rows, 1), 0)
    own = jnp.where(pos + parity * rows < length, 0.0, mask_fill)
    other = jnp.where(pos + (1 - parity) * rows < length, 0.0, mask_fill)
    return own, other


def turned(array, lane):
    low = lane % HEAD_DIM < HEAD_DIM // 2
    return jnp.where(
        low, pltpu.roll(array, PAIR - HEAD_DIM // 2, 1), pltpu.roll(array, HEAD_DIM // 2, 1)
    )


def qkv_kernel(n_ref, w_ref, b_ref, cos_ref, sin_ref, out_ref):
    part = pl.program_id(0)
    lane = lax.broadcasted_iota(jnp.int32, (1, PAIR), 1)
    width = w_ref.shape[0]
    flat = dot(n_ref[...], w_ref[...], 1, 1) + b_ref[0]

    @pl.when(part == 2)
    def _():
        out_ref[...] = flat.astype(bf16)

    @pl.when(part < 2)
    def _():
        scale = jnp.where(part == 0, HEAD_DIM**-0.5, 1.0).astype(f32)
        for start in range(0, width, PAIR):
            piece = flat[:, start : start + PAIR]
            piece = piece * cos_ref[...] + turned(piece, lane) * sin_ref[...]
            out_ref[:, pl.ds(start, PAIR)] = (piece * scale).astype(bf16)


def finish_kernel(dq_ref, dk_ref, dv_ref, gk_ref, gv_ref, cos_ref, sin_ref, out_ref, sum_ref):
    rows, width = dq_ref.shape
    lane = lax.broadcasted_iota(jnp.int32, (1, PAIR), 1)
    for part in range(3):
        for start in range(0, width, PAIR):
            cut = pl.ds(start, PAIR)
            if part == 0:
                piece = dq_ref[:, cut] * HEAD_DIM**-0.5
            elif part == 1:
                piece = dk_ref[:, cut] + gk_ref[:, cut].astype(f32)
            else:
                piece = dv_ref[:, cut] + gv_ref[:, cut].astype(f32)
            if part < 2:
                piece = piece * cos_ref[...] - turned(piece, lane) * sin_ref[...]
            piece = piece.astype(bf16)
            out_ref[:, pl.ds(part * width + start, PAIR)] = piece
            total = jnp.sum(piece.astype(f32), axis=0, keepdims=True)
            sum_ref[:, pl.ds(part * width + start, PAIR)] = jnp.broadcast_to(total, (8, PAIR))


def attend_fwd_kernel(info_ref, q_ref, ko_ref, vo_ref, kp_ref, vp_ref, o_ref, lse_ref, vt_ref):
    rows = q_ref.shape[0]
    bias_own, bias_other = key_bias(info_ref, rows)
    lane = lax.broadcasted_iota(jnp.int32, (1, PAIR), 1)
    lse_ref[...] = jnp.zeros_like(lse_ref)
    vt_ref[0] = vo_ref[...].T
    vt_ref[1] = vp_ref[...].T
    for start in range(0, rows, TILE):
        q = q_ref[pl.ds(start, TILE), :]
        outs = []
        for head in range(2):
            in_head = (lane < HEAD_DIM) if head == 0 else (lane >= HEAD_DIM)
            own_rows = pl.ds(head * HEAD_DIM, HEAD_DIM)
            qm = jnp.where(in_head, q, jnp.zeros_like(q))
            s_own = dot(ko_ref[...], qm, 1, 1) + bias_own
            s_other = dot(kp_ref[...], qm, 1, 1) + bias_other
            top = jnp.maximum(
                jnp.max(s_own, axis=0, keepdims=True), jnp.max(s_other, axis=0, keepdims=True)
            )
            e_own = jnp.exp(s_own - top)
            e_other = jnp.exp(s_other - top)
            total = jnp.sum(e_own, axis=0, keepdims=True) + jnp.sum(e_other, axis=0, keepdims=True)
            lse_ref[0, pl.ds(head, 1), pl.ds(start, TILE)] = top + jnp.log(total)
            out = dot(vt_ref[0, own_rows, :], e_own.astype(bf16), 1, 0) + dot(
                vt_ref[1, own_rows, :], e_other.astype(bf16), 1, 0
            )
            outs.append(out * (1.0 / total))
        o_ref[pl.ds(start, TILE), :] = jnp.concatenate(outs, axis=0).T.astype(bf16)


def attend_bwd_kernel(
    info_ref, q_ref, ko_ref, vo_ref, kp_ref, vp_ref, do_ref, lse_ref,
    dq_ref, dko_ref, dvo_ref, dkp_ref, dvp_ref, dk_acc, dv_acc, kt_ref,
):
    rows = q_ref.shape[0]
    biases = key_bias(info_ref, rows)
    lane = lax.broadcasted_iota(jnp.int32, (1, PAIR), 1)
    kt_ref[0] = ko_ref[...].T
    kt_ref[1] = kp_ref[...].T
    for start in range(0, rows, TILE):
        q = q_ref[pl.ds(start, TILE), :]
        do = do_ref[pl.ds(start, TILE), :]
        dqs = []
        for head in range(2):
            in_head = (lane < HEAD_DIM) if head == 0 else (lane >= HEAD_DIM)
            own_rows = pl.ds(head * HEAD_DIM, HEAD_DIM)
            qm = jnp.where(in_head, q, jnp.zeros_like(q))
            dom = jnp.where(in_head, do, jnp.zeros_like(do))
            lse = lse_ref[0, pl.ds(head, 1), pl.ds(start, TILE)]
            probs, d_probs = [], []
            for bias, k_ref, v_ref in ((biases[0], ko_ref, vo_ref), (biases[1], kp_ref, vp_ref)):
                probs.append(jnp.exp(dot(k_ref[...], qm, 1, 1) + bias - lse))
                d_probs.append(dot(v_ref[...], dom, 1, 1))
            delta = jnp.sum(probs[0] * d_probs[0], axis=0, keepdims=True) + jnp.sum(
                probs[1] * d_probs[1], axis=0, keepdims=True
            )
            dq = None
            for side in range(2):
                ds = (probs[side] * (d_probs[side] - delta)).astype(bf16)
                dv = dot(probs[side].astype(bf16), dom, 1, 0)
                dk = dot(ds, qm, 1, 0)
                if start == 0 and head == 0:
                    dk_acc[side] = dk
                    dv_acc[side] = dv
                else:
                    dk_acc[side] += dk
                    dv_acc[side] += dv
                part = dot(kt_ref[side, own_rows, :], ds, 1, 0)
                dq = part if dq is None else dq + part
            dqs.append(dq)
        dq_ref[pl.ds(start, TILE), :] = jnp.concatenate(dqs, axis=0).T
    dko_ref[...] = dk_acc[0]
    dkp_ref[...] = dk_acc[1].astype(bf16)
    dvo_ref[...] = dv_acc[0]
    dvp_ref[...] = dv_acc[1].astype(bf16)


def cost(flops, bytes_accessed, transcendentals=0):
    return pl.CostEstimate(
        flops=flops, bytes_accessed=bytes_accessed, transcendentals=transcendentals
    )


def project_qkv(normed, weights, bias, cosine, sine):
    rows, model = normed.shape
    width = weights.shape[0] // 3
    whole = pl.BlockSpec((rows, PAIR), lambda c: (0, 0))
    return pl.pallas_call(
        qkv_kernel,
        grid=(3,),
        in_specs=[
            pl.BlockSpec((rows, model), lambda c: (0, 0)),
            pl.BlockSpec((width, model), lambda c: (c, 0)),
            pl.BlockSpec((1, 1, width), lambda c: (c, 0, 0)),
            whole,
            whole,
        ],
        out_specs=pl.BlockSpec((rows, width), lambda c: (0, c)),
        out_shape=jax.ShapeDtypeStruct((rows, 3 * width), bf16),
        cost_estimate=cost(6 * rows * model * width, 2 * (rows + 3 * width) * model),
        name="project_qkv",
    )(normed, weights, bias, cosine, sine)


def finish_qkv(dq, dk, dv, gk, gv, cosine, sine):
    rows, width = dq.shape
    return pl.pallas_call(
        finish_kernel,
        out_shape=[
            jax.ShapeDtypeStruct((rows, 3 * width), bf16),
            jax.ShapeDtypeStruct((8, 3 * width), f32),
        ],
        cost_estimate=cost(20 * rows * width, 24 * rows * width),
        name="finish_qkv",
    )(dq, dk, dv, gk, gv, cosine, sine)


def lanes(rows, offset):
    return pl.BlockSpec((rows, PAIR), lambda i, info: (0, offset + i))


def attend_fwd(info, qkv, other):
    rows, width = qkv.shape[0], qkv.shape[1] // 3
    pairs = width // PAIR
    stat = pl.BlockSpec((1, 8, rows), lambda i, info: (i, 0, 0))
    score = rows * rows * 2 * width
    return pl.pallas_call(
        attend_fwd_kernel,
        grid_spec=pltpu.PrefetchScalarGridSpec(
            num_scalar_prefetch=1,
            grid=(pairs,),
            in_specs=[lanes(rows, k) for k in (0, pairs, 2 * pairs, 0, pairs)],
            out_specs=[lanes(rows, 0), stat],
            scratch_shapes=[pltpu.VMEM((2, PAIR, rows), bf16)],
        ),
        out_shape=[
            jax.ShapeDtypeStruct((rows, width), bf16),
            jax.ShapeDtypeStruct((pairs, 8, rows), f32),
        ],
        cost_estimate=cost(8 * score, 12 * rows * width, score // HEAD_DIM),
        name="attend_fwd",
    )(info, qkv, qkv, qkv, other, other)


def attend_bwd(info, qkv, other, do, lse):
    rows, width = do.shape
    pairs = width // PAIR
    stat = pl.BlockSpec((1, 8, rows), lambda i, info: (i, 0, 0))
    score = rows * rows * 2 * width
    wide = jax.ShapeDtypeStruct((rows, width), f32)
    low = jax.ShapeDtypeStruct((rows, width), bf16)
    return pl.pallas_call(
        attend_bwd_kernel,
        grid_spec=pltpu.PrefetchScalarGridSpec(
            num_scalar_prefetch=1,
            grid=(pairs,),
            in_specs=[lanes(rows, k) for k in (0, pairs, 2 * pairs, 0, pairs, 0)] + [stat],
            out_specs=[lanes(rows, 0)] * 5,
            scratch_shapes=[pltpu.VMEM((2, rows, PAIR), f32)] * 2
            + [pltpu.VMEM((2, PAIR, rows), bf16)],
        ),
        out_shape=[wide, wide, wide, low, low],
        cost_estimate=cost(20 * score, 26 * rows * width, score // HEAD_DIM),
        name="attend_bwd",
    )(info, qkv, qkv, qkv, other, other, do, lse)


def local(
    tokens, seq_lengths, cotangent, ln1_gain, ln1_shift, w_qkv, b_qkv, w_out, b_out,
    ln2_gain, ln2_shift, w_up, b_up, w_down, b_down,
):
    rows, model = tokens.shape
    shard = w_qkv.shape[2]
    hidden = w_up.shape[1]
    half = 2 * shard
    me = lax.axis_index("tensor")
    parity = me % 2
    length = lax.dynamic_index_in_dim(seq_lengths, me // 2, 0, keepdims=False)
    info = jnp.stack([length, parity]).astype(jnp.int32)
    pad = 16

    def core(array):
        return swap(array, "tensor", 1)

    def far(array):
        return swap(array, "tensor", 2)

    def ordered(own, other, axis):
        first = jnp.where(parity == 0, own, other)
        second = jnp.where(parity == 0, other, own)
        return jnp.stack([first, second], axis=axis)

    flat = 3 * shard
    bias_rows = jnp.pad(b_qkv.reshape(1, flat), ((0, pad - 1), (0, model - flat)))
    attn_own = jnp.concatenate([w_qkv.transpose(1, 2, 0).reshape(flat, model), bias_rows], axis=0)
    attn_far = far(attn_own)
    bulk_far = far(jnp.concatenate([w_out, cotangent], axis=0))
    attn_core = core(attn_own)
    up_rows = jnp.broadcast_to(b_up.reshape(1, hidden), (pad, hidden))
    ffn_core = core(jnp.concatenate([w_up, up_rows, w_down, w_out], axis=0))
    out_far = bulk_far[:shard]
    cot_far = bulk_far[shard:]

    def join_qkv(own, other):
        weights = ordered(
            own[:flat].reshape(3, shard, model), other[:flat].reshape(3, shard, model), 1
        ).reshape(3 * half, model)
        bias = ordered(
            own[flat, :flat].reshape(3, shard), other[flat, :flat].reshape(3, shard), 1
        ).reshape(3, 1, half)
        return weights, bias.astype(f32)

    wq_near, bq_near = join_qkv(attn_own, attn_core)
    up_core = ffn_core[:model]
    bup_core = ffn_core[model : model + 1]
    down_core = ffn_core[model + pad : model + pad + hidden]
    wo_near = ordered(w_out, ffn_core[model + pad + hidden :], 0).reshape(half, model)
    w_up2 = jnp.concatenate([w_up, up_core], axis=1)
    b_up2 = jnp.concatenate([b_up.reshape(1, hidden), bup_core], axis=1).astype(f32)
    w_down2 = jnp.concatenate([w_down, down_core], axis=0)

    half_dim = HEAD_DIM // 2
    lane = jnp.arange(PAIR)
    inverse_freq = jnp.exp((lane % half_dim).astype(f32) * (-2.0 * math.log(10000.0) / HEAD_DIM))
    positions = (jnp.arange(rows) + (parity * rows) % SEQ).astype(f32)
    angles = positions[:, None] * inverse_freq[None, :]
    cosine = jnp.cos(angles)
    sine = jnp.sin(angles) * jnp.where(lane % HEAD_DIM < half_dim, -1.0, 1.0)

    resid = tokens.astype(f32)
    gain_one, shift_one = ln1_gain.astype(f32), ln1_shift.astype(f32)
    gain_two, shift_two = ln2_gain.astype(f32), ln2_shift.astype(f32)
    xhat_one, scale_one = norm_stats(resid)
    normed_one = (xhat_one * gain_one + shift_one).astype(bf16)

    def attention(weights, bias):
        qkv = project_qkv(normed_one, weights, bias, cosine, sine)
        other = core(qkv[:, half:])
        out, lse = attend_fwd(info, qkv, other)
        return out, (qkv, other, lse)

    attn_near, saved_near = attention(wq_near, bq_near)
    attn_far, out_far, attn_near = lax.optimization_barrier((attn_far, out_far, attn_near))
    attn_cross, out_cross = core(attn_far), core(out_far)
    wq_far, bq_far = join_qkv(attn_far, attn_cross)
    wo_far = ordered(out_far, out_cross, 0).reshape(half, model)
    attn_away, saved_away = attention(wq_far, bq_far)
    mixed = (
        resid + dot(attn_near, wo_near, 1, 0) + dot(attn_away, wo_far, 1, 0) + b_out.astype(f32)
    )

    xhat_two, scale_two = norm_stats(mixed)
    normed_two = (xhat_two * gain_two + shift_two).astype(bf16)
    normed_two_far = far(normed_two)
    grad_out = cotangent.astype(f32)

    def feed(normed, cot):
        pre = dot(normed, w_up2, 1, 0) + b_up2
        act, back = jax.vjp(jax.nn.gelu, pre)
        act = act.astype(bf16)
        d_pre = back(dot(cot, w_down2, 1, 1))[0].astype(bf16)
        return act, d_pre

    act, d_pre = feed(normed_two, cotangent)
    d_norm_own = dot(d_pre, w_up2, 1, 1)
    ffn_own = dot(act, w_down2, 1, 0)
    act_far, d_pre_far = feed(normed_two_far, cot_far)
    d_norm_got = far(dot(d_pre_far, w_up2, 1, 1).astype(bf16))
    g_down = dot(act, cotangent, 0, 0) + dot(act_far, cot_far, 0, 0)
    g_up = dot(normed_two, d_pre, 0, 0) + dot(normed_two_far, d_pre_far, 0, 0)
    g_b_up = jnp.sum(d_pre.astype(f32), axis=0) + jnp.sum(d_pre_far.astype(f32), axis=0)
    got_down = core(g_down[hidden:].astype(bf16))
    got_up = core(g_up[:, hidden:].astype(bf16))
    up_order = bits_of("dp")
    down_order = up_order[1:] + up_order[:1]
    sum_down = Sum((g_down[:hidden] + got_down.astype(f32)).astype(bf16), up_order)
    sum_up = Sum((g_up[:, :hidden] + got_up.astype(f32)).astype(bf16), down_order)
    ffn_sums = [sum_down, sum_up]
    d_norm_got, act_far = lax.optimization_barrier((d_norm_got, act_far))
    ffn_got = far(dot(act_far, w_down2, 1, 0).astype(bf16))
    d_normed_two = d_norm_own + d_norm_got.astype(f32)
    d_mixed = grad_out + norm_back(d_normed_two, gain_two, xhat_two, scale_two)
    d_branch = d_mixed.astype(bf16)
    d_vals_near = dot(d_branch, wo_near, 1, 1).astype(bf16)
    d_vals_away = dot(d_branch, wo_far, 1, 1).astype(bf16)

    def attention_back(saved, d_vals):
        d_vals = advance(ffn_sums, d_vals)
        dq, dk, dv, dkp, dvp = attend_bwd(info, saved[0], saved[1], d_vals, saved[2])
        gk, gv = core(dkp), core(dvp)
        dq = advance(ffn_sums, dq)
        return finish_qkv(dq, dk, dv, gk, gv, cosine, sine)

    def own_and_core(d_qkv, attn):
        grad = dot(d_qkv, normed_one, 0, 0).reshape(3, 2, shard, model)
        g_out = dot(attn, d_branch, 0, 0).reshape(1, 2, shard, model)
        grad = jnp.concatenate([grad, g_out], axis=0)
        own = lax.dynamic_index_in_dim(grad, parity, 1, keepdims=False)
        other = lax.dynamic_index_in_dim(grad, 1 - parity, 1, keepdims=False).astype(bf16)
        return own.reshape(4 * shard, model), core(other.reshape(4 * shard, model))

    d_qkv_away, b_away = attention_back(saved_away, d_vals_away)
    own, got = own_and_core(d_qkv_away, attn_away)
    pair_sum = (own + got.astype(f32)).astype(bf16)
    pair_far = far(pair_sum)
    d_vals_near, pair_sum = lax.optimization_barrier((d_vals_near, pair_sum))
    mixed, d_qkv_away = lax.optimization_barrier((mixed, d_qkv_away))
    output = (mixed + ffn_own + ffn_got.astype(f32) + b_down.astype(f32)).astype(bf16)
    d_qkv_near, b_near = attention_back(saved_near, d_vals_near)
    own, got = own_and_core(d_qkv_near, attn_near)
    g_attn = (own + got.astype(f32) + pair_far.astype(f32)).astype(bf16)
    attn_sums = [Sum(g_attn[: 2 * shard], up_order), Sum(g_attn[2 * shard :], down_order)]
    d_qkv_near = advance(ffn_sums + attn_sums, d_qkv_near)

    d_normed_one = dot(d_qkv_near, wq_near, 1, 0) + dot(d_qkv_away, wq_far, 1, 0)
    grad_tokens = (d_mixed + norm_back(d_normed_one, gain_one, xhat_one, scale_one)).astype(bf16)

    slot = jnp.arange(4)[:, None]
    g_b_near = b_near[0].reshape(3, 2, shard)
    g_b_away = b_away[0].reshape(3, 2, shard)

    def place(vector, index):
        return jnp.where(slot == index, vector[None, :], 0.0)

    def third(pair, index):
        vector = lax.dynamic_index_in_dim(pair, index % 2, 1, keepdims=False)
        return jnp.pad(vector.reshape(flat), (0, model - flat))

    slots_up = place(g_b_up[:hidden], me) + place(g_b_up[hidden:], me ^ 1)
    slots_qkv = (
        place(third(g_b_near, me), me)
        + place(third(g_b_near, me ^ 1), me ^ 1)
        + place(third(g_b_away, me), me ^ 2)
        + place(third(g_b_away, me ^ 1), me ^ 3)
    )
    small = jnp.concatenate(
        [
            jnp.stack(
                [
                    jnp.sum(d_normed_one * xhat_one, axis=0),
                    jnp.sum(d_normed_one, axis=0),
                    jnp.sum(d_mixed, axis=0),
                    jnp.sum(d_normed_two * xhat_two, axis=0),
                    jnp.sum(d_normed_two, axis=0),
                    jnp.sum(grad_out, axis=0),
                ]
            ),
            slots_up,
            slots_qkv,
            jnp.zeros((2, model), f32),
        ],
        axis=0,
    )
    for axis, bit in [("tensor", 1), ("tensor", 2)] + [("dp", bit) for bit in up_order]:
        small = advance(ffn_sums + attn_sums, small + swap(small, axis, bit))
    while any(item.todo or item.flight for item in ffn_sums + attn_sums):
        small = advance(ffn_sums + attn_sums, small)
    g_attn = jnp.concatenate([item.array for item in attn_sums], axis=0).astype(f32)
    g_b_up_all = lax.dynamic_index_in_dim(small, 6 + me, 0, keepdims=False)
    g_b_qkv_all = lax.dynamic_index_in_dim(small, 10 + me, 0, keepdims=False)
    return (
        output,
        grad_tokens,
        small[0],
        small[1],
        g_attn[:flat].T.reshape(model, 3, shard),
        g_b_qkv_all[: 3 * shard].reshape(3, shard),
        g_attn[flat:],
        small[2],
        small[3],
        small[4],
        sum_up.array.astype(f32),
        g_b_up_all,
        sum_down.array.astype(f32),
        small[5],
    )


def solution(mesh):
    placed = (
        P(("dp", "tensor"), None),
        P("dp"),
        P(("dp", "tensor"), None),
        P(),
        P(),
        P(None, None, "tensor"),
        P(None, "tensor"),
        P("tensor", None),
        P(),
        P(),
        P(),
        P(None, "tensor"),
        P("tensor"),
        P("tensor", None),
        P(),
    )
    return jax.shard_map(
        local,
        mesh=mesh,
        in_specs=placed,
        out_specs=(
            P(("dp", "tensor"), None),
            P(("dp", "tensor"), None),
            P(),
            P(),
            P(None, None, "tensor"),
            P(None, "tensor"),
            P("tensor", None),
            P(),
            P(),
            P(),
            P(None, "tensor"),
            P("tensor"),
            P("tensor", None),
            P(),
        ),
        check_vma=False,
    )
```
